128 devices in a mesh: row: 8 (over y, z_lo), col: 16 (over z_hi, x, core).
Axes of the slice: x: 4, y: 4, z: 4 (z_hi: 2, z_lo: 2; z = z_hi * 2 + z_lo), core: 2. Of those that a mesh axis runs over, the one named last changes fastest.
Arguments:
- spectra: bfloat16 [16, 2048, 2048], P('row', None, 'col'), may hold values from -6 to 6
- coupling: float32 [16], replicated, may hold values from 0.2 to 1
Outputs:
- returned_spectra: bfloat16 [16, 2048, 2048], P('row', None, 'col')
The draws below stay inside these ranges and needn't reach their ends.
All inputs are finite; a program needn't handle non-finite values.
Results may differ from the reference program's by a relative error of at most 0.0079.
Values may be sent and summed in bfloat16 or wider, within the bound.
A program may use at most 128 MiB of HBM per device.

```python
import math
import jax
import jax.numpy as jnp
from jax import lax

FIELDS = 8
LEV = 2
NX = 3072
NY = 3072
M = 1024


def shard_levels(own_key, dims, split, least, high):
    gain, own = 1.0, jax.random.fold_in(own_key, 6)
    for dim, blocks in split:
        heights = jnp.exp(jax.random.uniform(jax.random.fold_in(own, dim), (blocks,), jnp.float32, least / len(split), high / len(split)))
        gain = gain * jnp.repeat(heights, dims[dim] // blocks).reshape([-1 if axis == dim else 1 for axis in range(len(dims))])
    return gain


def scatter_about(stream_key, dims, scale, limit, shards=(), kind=jnp.bfloat16):
    array = scale * jax.random.normal(stream_key, dims, jnp.float32)
    if shards:
        array = array * shard_levels(stream_key, dims, shards, -0.22, 0.18)
    return jnp.clip(array, -limit, limit).astype(kind)


def setup_inputs(seed: int = 0) -> dict:
    seeds = jax.random.split(jax.random.key(seed), 3)
    spectra = scatter_about(seeds[0], (FIELDS * LEV, 2 * M, 2 * M), 1.0, 6.0, ((0, 8), (2, 16)))
    coupling = jnp.clip(jnp.exp(jax.random.uniform(seeds[1], (FIELDS * LEV,), jnp.float32, math.log(0.2), math.log(1.0))), 0.2, 1.0)
    return dict(spectra=spectra, coupling=coupling)


def fourier_rows(mode_count, length, factor):
    wavenumber = jnp.arange(1, mode_count + 1, dtype=jnp.int32)
    position = jnp.arange(length, dtype=jnp.int32)
    residue = wavenumber[:, None] * position[None, :] % length
    angles = residue.astype(jnp.float32) * (2.0 * math.pi / length)
    table = jnp.concatenate([jnp.cos(angles), jnp.sin(angles)], 0) * factor
    return table.astype(jnp.bfloat16)

def ellipse(row_index, column_index, mode_count):
    row_waves = row_index % mode_count + 1
    col_waves = column_index % mode_count + 1
    inside = row_waves[:, None] * row_waves[:, None] + col_waves[None, :] * col_waves[None, :] <= mode_count * mode_count
    return inside.astype(jnp.float32)

def reference(spectra, coupling):
    inverse_y = fourier_rows(M, NY, 1.0 / math.sqrt(M)).T
    inverse_x = fourier_rows(M, NX, 1.0 / math.sqrt(M))
    forward_x = fourier_rows(M, NX, 2.0 * math.sqrt(M) / NX).T
    forward_y = fourier_rows(M, NY, 2.0 * math.sqrt(M) / NY)
    modes = jnp.arange(2 * M, dtype=jnp.int32)
    inside = ellipse(modes, modes, M)

    def one_field(bundle):
        spectrum, strength = bundle
        half_done = jnp.dot(inverse_y, spectrum, preferred_element_type=jnp.float32).astype(jnp.bfloat16)
        gridded = jnp.dot(half_done, inverse_x, preferred_element_type=jnp.float32)
        tendency = (gridded + strength * gridded * gridded).astype(jnp.bfloat16)
        projected = jnp.dot(tendency, forward_x, preferred_element_type=jnp.float32).astype(jnp.bfloat16)
        result = jnp.dot(forward_y, projected, preferred_element_type=jnp.float32)
        return (result * inside).astype(jnp.bfloat16)
    return lax.map(one_field, (spectra, coupling))
```

```python
import functools
import math

import jax
import jax.numpy as jnp
import ml_dtypes
import numpy as np
from jax import lax
from jax.experimental import pallas as pl
from jax.experimental.pallas import tpu as pltpu
from jax.sharding import PartitionSpec as P

MESH = pl.DeviceIdType.MESH
N = 3072
M = 1024
MODES = 2 * M
NQ = 3
LINES = N // (16 * NQ)
ROWS = 16 * LINES
TILE = 256


def fourier_table():
    point = np.arange(N, dtype=np.int64)
    wave = np.arange(1, M + 1, dtype=np.int64)
    angle = (point[:, None] * wave[None, :] % N).astype(np.float64) * (2.0 * math.pi / N)
    table = np.concatenate([np.cos(angle), np.sin(angle)], 1) / math.sqrt(M)
    return table.astype(ml_dtypes.bfloat16)


def device_at(y, z, x, core):
    return (y * 2 + z % 2, z // 2 * 8 + x * 2 + core)


def round_trip(
    coupling, spectra, by_point, by_mode, out,
    spec, points, modes, sent1, got1, lines, tend, sent2, got2, total,
    load_sem, send_sem, recv_sem,
):
    row, col = lax.axis_index("row"), lax.axis_index("col")
    y, parity = row // 2, row % 2
    z_hi, x, core = col // 8, col // 2 % 4, col % 2
    other = 1 - parity
    mine = x * 4 + z_hi * 2 + core

    def partner(xp, zp, cp):
        return device_at(y, zp * 2 + other, xp, cp)

    loads = [
        pltpu.make_async_copy(spectra.at[f], spec.at[:, pl.ds(f * 128, 128)], load_sem.at[f])
        for f in range(2)
    ]
    loads += [
        pltpu.make_async_copy(
            by_point.at[pl.ds(q * ROWS, ROWS)], points.at[pl.ds(q * ROWS, ROWS)], load_sem.at[2 + q]
        )
        for q in range(NQ)
    ]
    loads.append(pltpu.make_async_copy(by_mode, modes, load_sem.at[2 + NQ]))
    for load in loads:
        load.start()

    barrier = pltpu.get_barrier_semaphore()
    for xp in range(4):
        for zp in range(2):
            for cp in range(2):
                pl.semaphore_signal(
                    barrier, inc=1, device_id=partner(xp, zp, cp), device_id_type=MESH
                )
    pl.semaphore_wait(barrier, 16)
    loads[0].wait()
    loads[1].wait()

    def whole(leg, q):
        sent, got = ((sent1, got1), (sent2, got2))[leg]
        return pltpu.make_async_remote_copy(
            sent.at[q], got.at[q], send_sem.at[leg, q], recv_sem.at[leg, q],
            device_id=partner(x, 0, core), device_id_type=MESH,
        )

    for q in range(NQ):
        loads[2 + q].wait()

        @pl.loop(0, 4)
        def _(i):
            xo = (x + 2 + 3 * i) % 4
            start = pl.multiple_of(q * ROWS + xo * 4 * LINES, 4 * LINES)
            half = jnp.dot(
                points[pl.ds(start, 4 * LINES), :], spec[...], preferred_element_type=jnp.float32
            ).astype(jnp.bfloat16)
            sent1[q, pl.ds(xo * 4, 4)] = half.reshape(4, LINES, 256)
            for zo in range(2):
                for co in range(2):
                    pltpu.make_async_remote_copy(
                        sent1.at[q, xo * 4 + zo * 2 + co], got1.at[q, col],
                        send_sem.at[0, q], recv_sem.at[0, q],
                        device_id=partner(xo, zo, co), device_id_type=MESH,
                    ).start()

    loads[2 + NQ].wait()
    field = (y * 2 + other) * 2
    strengths = (coupling[field], coupling[field + 1])

    for q in range(NQ):
        whole(0, q).wait_recv()
        for f in range(2):
            for s in range(16):
                lines[f * LINES : (f + 1) * LINES, s * 128 : (s + 1) * 128] = got1[
                    q, s, :, f * 128 : (f + 1) * 128
                ]

        @pl.loop(0, N // TILE)
        def _(n):
            cols = pl.ds(pl.multiple_of(n * TILE, TILE), TILE)
            grid = jnp.dot(lines[...], modes[:, cols], preferred_element_type=jnp.float32)
            for f in range(2):
                g = grid[f * LINES : (f + 1) * LINES]
                tend[f * LINES : (f + 1) * LINES, cols] = (g + strengths[f] * g * g).astype(
                    jnp.bfloat16
                )

        @pl.loop(0, 8)
        def _(i):
            zd, xd = i % 2, (x + 2 + 3 * (i // 2)) % 4
            n = zd * 4 + xd
            cols = pl.ds(pl.multiple_of(n * TILE, TILE), TILE)
            back = jnp.dot(tend[...], points[:, cols], preferred_element_type=jnp.float32)
            back = (back * (2.0 / 3.0)).astype(jnp.bfloat16)
            for cd in range(2):
                for f in range(2):
                    sent2[q, 2 * n + cd, :, f * 128 : (f + 1) * 128] = back[
                        f * LINES : (f + 1) * LINES, cd * 128 : (cd + 1) * 128
                    ]
                pltpu.make_async_remote_copy(
                    sent2.at[q, 2 * n + cd], got2.at[q, mine],
                    send_sem.at[1, q], recv_sem.at[1, q],
                    device_id=partner(xd, zd, cd), device_id_type=MESH,
                ).start()

    for q in range(NQ):
        whole(1, q).wait_recv()

        @pl.loop(0, MODES // TILE)
        def _(m):
            rows = pl.ds(pl.multiple_of(m * TILE, TILE), TILE)
            part = jnp.dot(
                modes[rows, q * ROWS : (q + 1) * ROWS],
                got2[q].reshape(ROWS, 256),
                preferred_element_type=jnp.float32,
            )
            if q > 0:
                part = part + total[rows, :]
            if q < NQ - 1:
                total[rows, :] = part
            else:
                part = (part * (2.0 / 3.0)).astype(jnp.bfloat16)
                for f in range(2):
                    out[f, rows, :] = part[:, f * 128 : (f + 1) * 128]

    for q in range(NQ):
        whole(0, q).wait_send()
        whole(1, q).wait_send()


def on_device(spectra, coupling):
    table = fourier_table()
    width = spectra.shape[2]
    anywhere = pl.BlockSpec(memory_space=pl.ANY)
    result = pl.pallas_call(
        round_trip,
        out_shape=jax.ShapeDtypeStruct(spectra.shape, jnp.bfloat16),
        in_specs=[pl.BlockSpec(memory_space=pltpu.SMEM), anywhere, anywhere, anywhere],
        out_specs=pl.BlockSpec(memory_space=pltpu.VMEM),
        scratch_shapes=[
            pltpu.VMEM((MODES, 256), jnp.bfloat16),
            pltpu.VMEM((N, MODES), jnp.bfloat16),
            pltpu.VMEM((MODES, N), jnp.bfloat16),
            pltpu.VMEM((NQ, 16, LINES, 256), jnp.bfloat16),
            pltpu.VMEM((NQ, 16, LINES, 256), jnp.bfloat16),
            pltpu.VMEM((2 * LINES, MODES), jnp.bfloat16),
            pltpu.VMEM((2 * LINES, N), jnp.bfloat16),
            pltpu.VMEM((NQ, 16, LINES, 256), jnp.bfloat16),
            pltpu.VMEM((NQ, 16, LINES, 256), jnp.bfloat16),
            pltpu.VMEM((MODES, 256), jnp.float32),
            pltpu.SemaphoreType.DMA((3 + NQ,)),
            pltpu.SemaphoreType.DMA((2, NQ)),
            pltpu.SemaphoreType.DMA((2, NQ)),
        ],
        compiler_params=pltpu.CompilerParams(
            collective_id=0, has_side_effects=True, vmem_limit_bytes=58 * 1024 * 1024
        ),
        cost_estimate=pl.CostEstimate(
            flops=16_000_000_000, bytes_accessed=30_000_000, transcendentals=0
        ),
    )(coupling, spectra, table, np.ascontiguousarray(table.T))
    kx = (lax.axis_index("col") * width + jnp.arange(width, dtype=jnp.int32)) % M + 1
    ky = jnp.arange(MODES, dtype=jnp.int32) % M + 1
    inside = ky[:, None] * ky[:, None] + kx[None, :] * kx[None, :] <= M * M
    return jnp.where(inside[None], result, jnp.zeros_like(result))


def solution(mesh):
    return jax.shard_map(
        on_device,
        mesh=mesh,
        in_specs=(P("row", None, "col"), P()),
        out_specs=P("row", None, "col"),
        check_vma=False,
    )
```

```python
import functools
import math

import jax
import jax.numpy as jnp
import ml_dtypes
import numpy as np
from jax import lax
from jax.experimental import pallas as pl
from jax.experimental.pallas import tpu as pltpu
from jax.sharding import PartitionSpec as P

MESH = pl.DeviceIdType.MESH
N = 3072
M = 1024
MODES = 2 * M
NQ = 3
LINES = N // (16 * NQ)
ROWS = 16 * LINES
TILE = 256


def fourier_table():
    point = np.arange(N, dtype=np.int64)
    wave = np.arange(1, M + 1, dtype=np.int64)
    angle = (point[:, None] * wave[None, :] % N).astype(np.float64) * (2.0 * math.pi / N)
    table = np.concatenate([np.cos(angle), np.sin(angle)], 1) / math.sqrt(M)
    return table.astype(ml_dtypes.bfloat16)


def device_at(y, z, x, core):
    return (y * 2 + z % 2, z // 2 * 8 + x * 2 + core)


def round_trip(
    coupling_hbm, spectra, by_point, by_mode, out,
    coupling, spec, points, modes, sent1, got1, lines, tend, sent2, got2, total,
    load_sem, send_sem, recv_sem, last_sem,
):
    row, col = lax.axis_index("row"), lax.axis_index("col")
    y, parity = row // 2, row % 2
    z_hi, x, core = col // 8, col // 2 % 4, col % 2
    other = 1 - parity
    mine = x * 4 + z_hi * 2 + core

    def partner(xp, zp, cp):
        return device_at(y, zp * 2 + other, xp, cp)

    loads = [
        pltpu.make_async_copy(spectra.at[f], spec.at[:, pl.ds(f * 128, 128)], load_sem.at[f])
        for f in range(2)
    ]
    for i in range(4):
        first = pl.ds(pl.multiple_of((x + 2 + 3 * i) % 4 * 4 * LINES, 4 * LINES), 4 * LINES)
        loads.append(
            pltpu.make_async_copy(by_point.at[first], points.at[first], load_sem.at[2 + i])
        )
    loads += [
        pltpu.make_async_copy(
            by_point.at[pl.ds(q * ROWS, ROWS)], points.at[pl.ds(q * ROWS, ROWS)], load_sem.at[5 + q]
        )
        for q in range(1, NQ)
    ]
    loads.append(pltpu.make_async_copy(by_mode, modes, load_sem.at[5 + NQ]))
    loads.append(pltpu.make_async_copy(coupling_hbm, coupling, load_sem.at[6 + NQ]))
    for load in loads:
        load.start()

    barrier = pltpu.get_barrier_semaphore()
    for xp in range(4):
        for zp in range(2):
            for cp in range(2):
                pl.semaphore_signal(
                    barrier, inc=1, device_id=partner(xp, zp, cp), device_id_type=MESH
                )
    pl.semaphore_wait(barrier, 16)
    loads[0].wait()
    loads[1].wait()

    def whole(leg, q):
        sent, got = ((sent1, got1), (sent2, got2))[leg]
        return pltpu.make_async_remote_copy(
            sent.at[q], got.at[q], send_sem.at[leg, q], recv_sem.at[leg, q],
            device_id=partner(x, 0, core), device_id_type=MESH,
        )

    def last_part(xs):
        return pltpu.make_async_remote_copy(
            sent2.at[NQ - 1, pl.ds(0, 4)], got2.at[NQ - 1, pl.ds(xs * 4, 4)],
            send_sem.at[1, NQ - 1], last_sem.at[xs],
            device_id=partner(x, 0, core), device_id_type=MESH,
        )

    def to_rows(q, i):
        xo = (x + 2 + 3 * i) % 4
        start = pl.multiple_of(q * ROWS + xo * 4 * LINES, 4 * LINES)
        half = jnp.dot(
            points[pl.ds(start, 4 * LINES), :], spec[...], preferred_element_type=jnp.float32
        ).astype(jnp.bfloat16)
        sent1[q, pl.ds(xo * 4, 4)] = half.reshape(4, LINES, 256)

    def send_rows(q, i):
        xo = (x + 2 + 3 * i) % 4
        for zo in range(2):
            for co in range(2):
                pltpu.make_async_remote_copy(
                    sent1.at[q, xo * 4 + zo * 2 + co], got1.at[q, col],
                    send_sem.at[0, q], recv_sem.at[0, q],
                    device_id=partner(xo, zo, co), device_id_type=MESH,
                ).start()

    for q in range(NQ):
        if q == 0:
            for i in range(4):
                loads[2 + i].wait()
                to_rows(q, i)
                send_rows(q, i)
        else:
            loads[5 + q].wait()
            for i in range(4):
                to_rows(q, i)

            @pl.loop(0, 4)
            def _(i):
                send_rows(q, i)

    loads[5 + NQ].wait()
    loads[6 + NQ].wait()
    field = (y * 2 + other) * 2
    strengths = (coupling[field], coupling[field + 1])

    for q in range(NQ):
        whole(0, q).wait_recv()
        for f in range(2):
            for s in range(16):
                lines[f * LINES : (f + 1) * LINES, s * 128 : (s + 1) * 128] = got1[
                    q, s, :, f * 128 : (f + 1) * 128
                ]

        @pl.loop(0, N // TILE, unroll=4)
        def _(n):
            cols = pl.ds(pl.multiple_of(n * TILE, TILE), TILE)
            grid = jnp.dot(lines[...], modes[:, cols], preferred_element_type=jnp.float32)
            for f in range(2):
                g = grid[f * LINES : (f + 1) * LINES]
                tend[f * LINES : (f + 1) * LINES, cols] = (g + strengths[f] * g * g).astype(
                    jnp.bfloat16
                )

        def to_modes(i):
            zd, xd = i % 2, (x + 2 + 3 * (i // 2)) % 4
            n = zd * 4 + xd
            cols = pl.ds(pl.multiple_of(n * TILE, TILE), TILE)
            back = jnp.dot(tend[...], points[:, cols], preferred_element_type=jnp.float32)
            back = (back * (2.0 / 3.0)).astype(jnp.bfloat16)
            for cd in range(2):
                for f in range(2):
                    sent2[q, 2 * n + cd, :, f * 128 : (f + 1) * 128] = back[
                        f * LINES : (f + 1) * LINES, cd * 128 : (cd + 1) * 128
                    ]

        def send_modes(i):
            zd, xd = i % 2, (x + 2 + 3 * (i // 2)) % 4
            n = zd * 4 + xd
            for cd in range(2):
                pltpu.make_async_remote_copy(
                    sent2.at[q, 2 * n + cd], got2.at[q, mine],
                    send_sem.at[1, q], last_sem.at[x] if q == NQ - 1 else recv_sem.at[1, q],
                    device_id=partner(xd, zd, cd), device_id_type=MESH,
                ).start()

        @pl.loop(0, 2)
        def _(h):
            for i in range(4):
                to_modes(h * 4 + i)
            for i in range(4):
                send_modes(h * 4 + i)

    kx = (col * 128 + lax.broadcasted_iota(jnp.int32, (1, 128), 1)) % M + 1

    def finish(rows, start, part):
        part = (part * (2.0 / 3.0)).astype(jnp.bfloat16)
        ky = (start + lax.broadcasted_iota(jnp.int32, (TILE, 1), 0)) % M + 1
        inside = kx * kx + ky * ky <= M * M
        for f in range(2):
            kept = jnp.where(inside, part[:, f * 128 : (f + 1) * 128], 0.0)
            out[f, rows, :] = kept.astype(jnp.bfloat16)

    for q in range(NQ - 1):
        whole(1, q).wait_recv()

        @pl.loop(0, MODES // TILE, unroll=4)
        def _(m):
            rows = pl.ds(pl.multiple_of(m * TILE, TILE), TILE)
            part = jnp.dot(
                modes[rows, q * ROWS : (q + 1) * ROWS],
                got2[q].reshape(ROWS, 256),
                preferred_element_type=jnp.float32,
            )
            if q > 0:
                part = part + total[rows, :]
            total[rows, :] = part

    for j in range(4):
        xs = (x + 2 + j) % 4
        last_part(xs).wait_recv()
        cols = pl.ds(pl.multiple_of((NQ - 1) * ROWS + xs * 4 * LINES, 4 * LINES), 4 * LINES)

        @pl.loop(0, MODES // TILE, unroll=4)
        def _(m):
            start = pl.multiple_of(m * TILE, TILE)
            rows = pl.ds(start, TILE)
            part = total[rows, :] + jnp.dot(
                modes[rows, cols],
                got2[NQ - 1, pl.ds(xs * 4, 4)].reshape(4 * LINES, 256),
                preferred_element_type=jnp.float32,
            )
            if j < 3:
                total[rows, :] = part
            else:
                finish(rows, start, part)

    for q in range(NQ):
        whole(0, q).wait_send()
        whole(1, q).wait_send()


def on_device(spectra, coupling):
    table = fourier_table()
    in_hbm = pl.BlockSpec(memory_space=pltpu.HBM)
    return pl.pallas_call(
        round_trip,
        out_shape=jax.ShapeDtypeStruct(spectra.shape, jnp.bfloat16),
        in_specs=[in_hbm] * 4,
        out_specs=pl.BlockSpec(memory_space=pltpu.VMEM),
        scratch_shapes=[
            pltpu.SMEM((16,), jnp.float32),
            pltpu.VMEM((MODES, 256), jnp.bfloat16),
            pltpu.VMEM((N, MODES), jnp.bfloat16),
            pltpu.VMEM((MODES, N), jnp.bfloat16),
            pltpu.VMEM((NQ, 16, LINES, 256), jnp.bfloat16),
            pltpu.VMEM((NQ, 16, LINES, 256), jnp.bfloat16),
            pltpu.VMEM((2 * LINES, MODES), jnp.bfloat16),
            pltpu.VMEM((2 * LINES, N), jnp.bfloat16),
            pltpu.VMEM((NQ, 16, LINES, 256), jnp.bfloat16),
            pltpu.VMEM((NQ, 16, LINES, 256), jnp.bfloat16),
            pltpu.VMEM((MODES, 256), jnp.float32),
            pltpu.SemaphoreType.DMA((7 + NQ,)),
            pltpu.SemaphoreType.DMA((2, NQ)),
            pltpu.SemaphoreType.DMA((2, NQ)),
            pltpu.SemaphoreType.DMA((4,)),
        ],
        compiler_params=pltpu.CompilerParams(
            collective_id=0, has_side_effects=True, vmem_limit_bytes=48 * 1024 * 1024
        ),
        cost_estimate=pl.CostEstimate(
            flops=16_000_000_000, bytes_accessed=30_000_000, transcendentals=0
        ),
    )(*(pltpu.with_memory_space_constraint(a, pltpu.HBM) for a in (coupling, spectra)), table, np.ascontiguousarray(table.T))


def solution(mesh):
    return jax.shard_map(
        on_device,
        mesh=mesh,
        in_specs=(P("row", None, "col"), P()),
        out_specs=P("row", None, "col"),
        check_vma=False,
    )
```

```python
import functools
import math

import jax
import jax.numpy as jnp
import ml_dtypes
import numpy as np
from jax import lax
from jax.experimental import pallas as pl
from jax.experimental.pallas import tpu as pltpu
from jax.sharding import PartitionSpec as P

MESH = pl.DeviceIdType.MESH
N = 3072
M = 1024
MODES = 2 * M
EARLY = 1
NQ = 3
LINES = N // (16 * NQ)
ROWS = 16 * LINES
TILE = 256


def fourier_table():
    point = np.arange(N, dtype=np.int64)
    wave = np.arange(1, M + 1, dtype=np.int64)
    angle = (point[:, None] * wave[None, :] % N).astype(np.float64) * (2.0 * math.pi / N)
    table = np.concatenate([np.cos(angle), np.sin(angle)], 1) / math.sqrt(M)
    return table.astype(ml_dtypes.bfloat16)


def device_at(y, z, x, core):
    return (y * 2 + z % 2, z // 2 * 8 + x * 2 + core)


def round_trip(
    coupling_hbm, spectra, by_point, by_mode, out,
    coupling, spec, points, modes, sent1, got1, lines, tend, sent2, got2, total,
    load_sem, send_sem, recv_sem, last_sem,
):
    row, col = lax.axis_index("row"), lax.axis_index("col")
    y, parity = row // 2, row % 2
    z_hi, x, core = col // 8, col // 2 % 4, col % 2
    other = 1 - parity
    mine = x * 4 + z_hi * 2 + core
    z = z_hi * 2 + parity

    def x_at(i):
        return (x + (1, 3, 2, 0)[i]) % 4

    def z_at(up):
        return (z + 1 + 2 * (up % 2)) % 4 // 2

    def partner(xp, zp, cp):
        return device_at(y, zp * 2 + other, xp, cp)

    loads = [
        pltpu.make_async_copy(spectra.at[f], spec.at[:, pl.ds(f * 128, 128)], load_sem.at[f])
        for f in range(2)
    ]
    for i in range(4):
        first = pl.ds(pl.multiple_of(x_at(i) * 4 * LINES, 4 * LINES), 4 * LINES)
        loads.append(
            pltpu.make_async_copy(by_point.at[first], points.at[first], load_sem.at[2 + i])
        )
    loads += [
        pltpu.make_async_copy(
            by_point.at[pl.ds(q * ROWS, ROWS)], points.at[pl.ds(q * ROWS, ROWS)], load_sem.at[5 + q]
        )
        for q in range(1, NQ)
    ]
    loads.append(pltpu.make_async_copy(by_mode, modes, load_sem.at[5 + NQ]))
    loads.append(pltpu.make_async_copy(coupling_hbm, coupling, load_sem.at[6 + NQ]))
    for load in loads:
        load.start()

    barrier = pltpu.get_barrier_semaphore()
    for xp in range(4):
        for zp in range(2):
            for cp in range(2):
                pl.semaphore_signal(
                    barrier, inc=1, device_id=partner(xp, zp, cp), device_id_type=MESH
                )
    loads[0].wait()
    loads[1].wait()

    def whole(leg, q):
        sent, got = ((sent1, got1), (sent2, got2))[leg]
        return pltpu.make_async_remote_copy(
            sent.at[q], got.at[q], send_sem.at[leg, q], recv_sem.at[leg, q],
            device_id=partner(x, 0, core), device_id_type=MESH,
        )

    def last_part(xs):
        return pltpu.make_async_remote_copy(
            sent2.at[NQ - 1, pl.ds(0, 4)], got2.at[NQ - 1, pl.ds(xs * 4, 4)],
            send_sem.at[1, NQ - 1], last_sem.at[xs],
            device_id=partner(x, 0, core), device_id_type=MESH,
        )

    def to_rows(q, i):
        xo = x_at(i)
        start = pl.multiple_of(q * ROWS + xo * 4 * LINES, 4 * LINES)
        half = jnp.dot(
            points[pl.ds(start, 4 * LINES), :], spec[...], preferred_element_type=jnp.float32
        ).astype(jnp.bfloat16)
        sent1[q, pl.ds(xo * 4, 4)] = half.reshape(4, LINES, 256)

    def send_rows(q, i, up):
        xo, zo = x_at(i), z_at(up)
        for co in range(2):
            pltpu.make_async_remote_copy(
                sent1.at[q, xo * 4 + zo * 2 + co], got1.at[q, col],
                send_sem.at[0, q], recv_sem.at[0, q],
                device_id=partner(xo, zo, co), device_id_type=MESH,
            ).start()

    for i in range(EARLY):
        loads[2 + i].wait()
        to_rows(0, i)
    pl.semaphore_wait(barrier, 16)
    for up in range(2):
        for i in range(EARLY):
            send_rows(0, i, i + up)
    for i in range(EARLY, 4):
        loads[2 + i].wait()
        to_rows(0, i)
        send_rows(0, i, i)
        send_rows(0, i, i + 1)
    for q in range(1, NQ):
        loads[5 + q].wait()
        for i in range(4):
            to_rows(q, i)
        for up in range(2):
            for i in range(4):
                send_rows(q, i, i + up)

    loads[5 + NQ].wait()
    loads[6 + NQ].wait()
    field = (y * 2 + other) * 2
    strengths = (coupling[field], coupling[field + 1])

    for q in range(NQ):
        whole(0, q).wait_recv()
        for f in range(2):
            for s in range(16):
                lines[f * LINES : (f + 1) * LINES, s * 128 : (s + 1) * 128] = got1[
                    q, s, :, f * 128 : (f + 1) * 128
                ]

        @pl.loop(0, N // TILE, unroll=4)
        def _(n):
            cols = pl.ds(pl.multiple_of(n * TILE, TILE), TILE)
            grid = jnp.dot(lines[...], modes[:, cols], preferred_element_type=jnp.float32)
            for f in range(2):
                g = grid[f * LINES : (f + 1) * LINES]
                tend[f * LINES : (f + 1) * LINES, cols] = (g + strengths[f] * g * g).astype(
                    jnp.bfloat16
                )

        def to_modes(h, i):
            zd, xd = z_at(h + i), x_at(i)
            n = zd * 4 + xd
            cols = pl.ds(pl.multiple_of(n * TILE, TILE), TILE)
            back = jnp.dot(tend[...], points[:, cols], preferred_element_type=jnp.float32)
            back = (back * (2.0 / 3.0)).astype(jnp.bfloat16)
            for cd in range(2):
                for f in range(2):
                    sent2[q, 2 * n + cd, :, f * 128 : (f + 1) * 128] = back[
                        f * LINES : (f + 1) * LINES, cd * 128 : (cd + 1) * 128
                    ]

        def send_modes(h, i):
            zd, xd = z_at(h + i), x_at(i)
            n = zd * 4 + xd
            for cd in range(2):
                pltpu.make_async_remote_copy(
                    sent2.at[q, 2 * n + cd], got2.at[q, mine],
                    send_sem.at[1, q], last_sem.at[x] if q == NQ - 1 else recv_sem.at[1, q],
                    device_id=partner(xd, zd, cd), device_id_type=MESH,
                ).start()

        @pl.loop(0, 2)
        def _(h):
            for i in range(4):
                to_modes(h, i)
            for i in range(4):
                send_modes(h, i)

    kx = (col * 128 + lax.broadcasted_iota(jnp.int32, (1, 128), 1)) % M + 1

    def finish(rows, start, part):
        part = (part * (2.0 / 3.0)).astype(jnp.bfloat16)
        ky = (start + lax.broadcasted_iota(jnp.int32, (TILE, 1), 0)) % M + 1
        inside = kx * kx + ky * ky <= M * M
        for f in range(2):
            kept = jnp.where(inside, part[:, f * 128 : (f + 1) * 128], 0.0)
            out[f, rows, :] = kept.astype(jnp.bfloat16)

    for q in range(NQ - 1):
        whole(1, q).wait_recv()

        @pl.loop(0, MODES // TILE, unroll=4)
        def _(m):
            rows = pl.ds(pl.multiple_of(m * TILE, TILE), TILE)
            part = jnp.dot(
                modes[rows, q * ROWS : (q + 1) * ROWS],
                got2[q].reshape(ROWS, 256),
                preferred_element_type=jnp.float32,
            )
            if q > 0:
                part = part + total[rows, :]
            total[rows, :] = part

    for j in range(4):
        xs = (x + (3, 1, 2, 0)[j]) % 4
        last_part(xs).wait_recv()
        cols = pl.ds(pl.multiple_of((NQ - 1) * ROWS + xs * 4 * LINES, 4 * LINES), 4 * LINES)

        @pl.loop(0, MODES // TILE, unroll=4)
        def _(m):
            start = pl.multiple_of(m * TILE, TILE)
            rows = pl.ds(start, TILE)
            part = total[rows, :] + jnp.dot(
                modes[rows, cols],
                got2[NQ - 1, pl.ds(xs * 4, 4)].reshape(4 * LINES, 256),
                preferred_element_type=jnp.float32,
            )
            if j < 3:
                total[rows, :] = part
            else:
                finish(rows, start, part)

    for q in range(NQ):
        whole(0, q).wait_send()
        whole(1, q).wait_send()


def on_device(spectra, coupling):
    table = fourier_table()
    in_hbm = pl.BlockSpec(memory_space=pltpu.HBM)
    return pl.pallas_call(
        round_trip,
        out_shape=jax.ShapeDtypeStruct(spectra.shape, jnp.bfloat16),
        in_specs=[in_hbm] * 4,
        out_specs=pl.BlockSpec(memory_space=pltpu.VMEM),
        scratch_shapes=[
            pltpu.SMEM((16,), jnp.float32),
            pltpu.VMEM((MODES, 256), jnp.bfloat16),
            pltpu.VMEM((N, MODES), jnp.bfloat16),
            pltpu.VMEM((MODES, N), jnp.bfloat16),
            pltpu.VMEM((NQ, 16, LINES, 256), jnp.bfloat16),
            pltpu.VMEM((NQ, 16, LINES, 256), jnp.bfloat16),
            pltpu.VMEM((2 * LINES, MODES), jnp.bfloat16),
            pltpu.VMEM((2 * LINES, N), jnp.bfloat16),
            pltpu.VMEM((NQ, 16, LINES, 256), jnp.bfloat16),
            pltpu.VMEM((NQ, 16, LINES, 256), jnp.bfloat16),
            pltpu.VMEM((MODES, 256), jnp.float32),
            pltpu.SemaphoreType.DMA((7 + NQ,)),
            pltpu.SemaphoreType.DMA((2, NQ)),
            pltpu.SemaphoreType.DMA((2, NQ)),
            pltpu.SemaphoreType.DMA((4,)),
        ],
        compiler_params=pltpu.CompilerParams(
            collective_id=0, has_side_effects=True, vmem_limit_bytes=48 * 1024 * 1024
        ),
        cost_estimate=pl.CostEstimate(
            flops=16_000_000_000, bytes_accessed=30_000_000, transcendentals=0
        ),
    )(*(pltpu.with_memory_space_constraint(a, pltpu.HBM) for a in (coupling, spectra)), table, np.ascontiguousarray(table.T))


def solution(mesh):
    return jax.shard_map(
        on_device,
        mesh=mesh,
        in_specs=(P("row", None, "col"), P()),
        out_specs=P("row", None, "col"),
        check_vma=False,
    )
```

```python
import functools
import math

import jax
import jax.numpy as jnp
import ml_dtypes
import numpy as np
from jax import lax
from jax.experimental import pallas as pl
from jax.experimental.pallas import tpu as pltpu
from jax.sharding import PartitionSpec as P

MESH = pl.DeviceIdType.MESH
N = 3072
M = 1024
MODES = 2 * M
EARLY = 1
NQ = 3
LINES = N // (16 * NQ)
ROWS = 16 * LINES
TILE = 256


def fourier_table():
    point = np.arange(N, dtype=np.int64)
    wave = np.arange(1, M + 1, dtype=np.int64)
    angle = (point[:, None] * wave[None, :] % N).astype(np.float64) * (2.0 * math.pi / N)
    table = np.concatenate([np.cos(angle), np.sin(angle)], 1) / math.sqrt(M)
    return table.astype(ml_dtypes.bfloat16)


def device_at(y, z, x, core):
    return (y * 2 + z % 2, z // 2 * 8 + x * 2 + core)


def round_trip(
    coupling_hbm, spectra, by_point, by_mode, out,
    coupling, spec, points, modes, sent1, got1, lines, tend, sent2, got2, total,
    load_sem, send_sem, recv_sem, last_sem,
):
    row, col = lax.axis_index("row"), lax.axis_index("col")
    y, parity = row // 2, row % 2
    z_hi, x, core = col // 8, col // 2 % 4, col % 2
    other = 1 - parity
    mine = x * 4 + z_hi * 2 + core
    z = z_hi * 2 + parity

    def x_at(i):
        return (x + (1, 3, 2, 0)[i]) % 4

    def z_at(up):
        return (z + 1 + 2 * (up % 2)) % 4 // 2

    def partner(xp, zp, cp):
        return device_at(y, zp * 2 + other, xp, cp)

    loads = [
        pltpu.make_async_copy(spectra.at[f], spec.at[:, pl.ds(f * 128, 128)], load_sem.at[f])
        for f in range(2)
    ]
    for i in range(4):
        first = pl.ds(pl.multiple_of(x_at(i) * 4 * LINES, 4 * LINES), 4 * LINES)
        loads.append(
            pltpu.make_async_copy(by_point.at[first], points.at[first], load_sem.at[2 + i])
        )
    loads += [
        pltpu.make_async_copy(
            by_point.at[pl.ds(q * ROWS, ROWS)], points.at[pl.ds(q * ROWS, ROWS)], load_sem.at[5 + q]
        )
        for q in range(1, NQ)
    ]
    loads.append(pltpu.make_async_copy(by_mode, modes, load_sem.at[5 + NQ]))
    loads.append(pltpu.make_async_copy(coupling_hbm, coupling, load_sem.at[6 + NQ]))
    for load in loads:
        load.start()

    barrier = pltpu.get_barrier_semaphore()
    for xp in range(4):
        for zp in range(2):
            for cp in range(2):
                pl.semaphore_signal(
                    barrier, inc=1, device_id=partner(xp, zp, cp), device_id_type=MESH
                )
    loads[0].wait()
    loads[1].wait()

    def whole(leg, q):
        sent, got = ((sent1, got1), (sent2, got2))[leg]
        return pltpu.make_async_remote_copy(
            sent.at[q], got.at[q], send_sem.at[leg, q], recv_sem.at[leg, q],
            device_id=partner(x, 0, core), device_id_type=MESH,
        )

    def last_part(xs):
        return pltpu.make_async_remote_copy(
            sent2.at[NQ - 1, pl.ds(0, 4)], got2.at[NQ - 1, pl.ds(xs * 4, 4)],
            send_sem.at[1, NQ - 1], last_sem.at[xs],
            device_id=partner(x, 0, core), device_id_type=MESH,
        )

    def to_rows(q, i):
        xo = x_at(i)
        start = pl.multiple_of(q * ROWS + xo * 4 * LINES, 4 * LINES)
        half = jnp.dot(
            points[pl.ds(start, 4 * LINES), :], spec[...], preferred_element_type=jnp.float32
        ).astype(jnp.bfloat16)
        sent1[q, pl.ds(xo * 4, 4)] = half.reshape(4, LINES, 256)

    def send_rows(q, i, up):
        xo, zo = x_at(i), z_at(up)
        for co in range(2):
            pltpu.make_async_remote_copy(
                sent1.at[q, xo * 4 + zo * 2 + co], got1.at[q, col],
                send_sem.at[0, q], recv_sem.at[0, q],
                device_id=partner(xo, zo, co), device_id_type=MESH,
            ).start()

    for i in range(EARLY):
        loads[2 + i].wait()
        to_rows(0, i)
    pl.semaphore_wait(barrier, 16)
    for up in range(2):
        for i in range(EARLY):
            send_rows(0, i, i + up)
    for i in range(EARLY, 4):
        loads[2 + i].wait()
        to_rows(0, i)
        send_rows(0, i, i)
        send_rows(0, i, i + 1)
    for q in range(1, NQ):
        loads[5 + q].wait()
        for i in range(4):
            to_rows(q, i)
        for up in range(2):
            for i in range(4):
                send_rows(q, i, i + up)

    loads[5 + NQ].wait()
    loads[6 + NQ].wait()
    field = (y * 2 + other) * 2
    strengths = (coupling[field], coupling[field + 1])

    for q in range(NQ):
        whole(0, q).wait_recv()
        for f in range(2):
            for s in range(16):
                lines[f * LINES : (f + 1) * LINES, s * 128 : (s + 1) * 128] = got1[
                    q, s, :, f * 128 : (f + 1) * 128
                ]

        @pl.loop(0, N // TILE, unroll=4)
        def _(n):
            cols = pl.ds(pl.multiple_of(n * TILE, TILE), TILE)
            grid = jnp.dot(lines[...], modes[:, cols], preferred_element_type=jnp.float32)
            for f in range(2):
                g = grid[f * LINES : (f + 1) * LINES]
                tend[f * LINES : (f + 1) * LINES, cols] = (g + strengths[f] * g * g).astype(
                    jnp.bfloat16
                )

        def to_modes(h, i):
            zd, xd = z_at(h + i), x_at(i)
            n = zd * 4 + xd
            cols = pl.ds(pl.multiple_of(n * TILE, TILE), TILE)
            back = jnp.dot(tend[...], points[:, cols], preferred_element_type=jnp.float32)
            back = (back * (2.0 / 3.0)).astype(jnp.bfloat16)
            for cd in range(2):
                for f in range(2):
                    sent2[q, 2 * n + cd, :, f * 128 : (f + 1) * 128] = back[
                        f * LINES : (f + 1) * LINES, cd * 128 : (cd + 1) * 128
                    ]

        def send_modes(h, i):
            zd, xd = z_at(h + i), x_at(i)
            n = zd * 4 + xd
            for cd in (1, 0):
                pltpu.make_async_remote_copy(
                    sent2.at[q, 2 * n + cd], got2.at[q, mine],
                    send_sem.at[1, q], last_sem.at[x] if q == NQ - 1 else recv_sem.at[1, q],
                    device_id=partner(xd, zd, cd), device_id_type=MESH,
                ).start()

        @pl.loop(0, 2)
        def _(h):
            for pair in (0, 2):
                for i in range(2):
                    to_modes(h, pair + i)
                for i in range(2):
                    send_modes(h, pair + i)

    kx = (col * 128 + lax.broadcasted_iota(jnp.int32, (1, 128), 1)) % M + 1

    def finish(rows, start, part):
        part = (part * (2.0 / 3.0)).astype(jnp.bfloat16)
        ky = (start + lax.broadcasted_iota(jnp.int32, (TILE, 1), 0)) % M + 1
        inside = kx * kx + ky * ky <= M * M
        for f in range(2):
            kept = jnp.where(inside, part[:, f * 128 : (f + 1) * 128], 0.0)
            out[f, rows, :] = kept.astype(jnp.bfloat16)

    for q in range(NQ - 1):
        whole(1, q).wait_recv()

        @pl.loop(0, MODES // TILE, unroll=4)
        def _(m):
            rows = pl.ds(pl.multiple_of(m * TILE, TILE), TILE)
            part = jnp.dot(
                modes[rows, q * ROWS : (q + 1) * ROWS],
                got2[q].reshape(ROWS, 256),
                preferred_element_type=jnp.float32,
            )
            if q > 0:
                part = part + total[rows, :]
            total[rows, :] = part

    for j in range(4):
        xs = (x + (3, 1, 2, 0)[j]) % 4
        last_part(xs).wait_recv()
        cols = pl.ds(pl.multiple_of((NQ - 1) * ROWS + xs * 4 * LINES, 4 * LINES), 4 * LINES)

        @pl.loop(0, MODES // TILE, unroll=8)
        def _(m):
            start = pl.multiple_of(m * TILE, TILE)
            rows = pl.ds(start, TILE)
            part = total[rows, :] + jnp.dot(
                modes[rows, cols],
                got2[NQ - 1, pl.ds(xs * 4, 4)].reshape(4 * LINES, 256),
                preferred_element_type=jnp.float32,
            )
            if j < 3:
                total[rows, :] = part
            else:
                finish(rows, start, part)

    for q in range(NQ):
        whole(0, q).wait_send()
        whole(1, q).wait_send()


def on_device(spectra, coupling):
    table = fourier_table()
    in_hbm = pl.BlockSpec(memory_space=pltpu.HBM)
    return pl.pallas_call(
        round_trip,
        out_shape=jax.ShapeDtypeStruct(spectra.shape, jnp.bfloat16),
        in_specs=[in_hbm] * 4,
        out_specs=pl.BlockSpec(memory_space=pltpu.VMEM),
        scratch_shapes=[
            pltpu.SMEM((16,), jnp.float32),
            pltpu.VMEM((MODES, 256), jnp.bfloat16),
            pltpu.VMEM((N, MODES), jnp.bfloat16),
            pltpu.VMEM((MODES, N), jnp.bfloat16),
            pltpu.VMEM((NQ, 16, LINES, 256), jnp.bfloat16),
            pltpu.VMEM((NQ, 16, LINES, 256), jnp.bfloat16),
            pltpu.VMEM((2 * LINES, MODES), jnp.bfloat16),
            pltpu.VMEM((2 * LINES, N), jnp.bfloat16),
            pltpu.VMEM((NQ, 16, LINES, 256), jnp.bfloat16),
            pltpu.VMEM((NQ, 16, LINES, 256), jnp.bfloat16),
            pltpu.VMEM((MODES, 256), jnp.float32),
            pltpu.SemaphoreType.DMA((7 + NQ,)),
            pltpu.SemaphoreType.DMA((2, NQ)),
            pltpu.SemaphoreType.DMA((2, NQ)),
            pltpu.SemaphoreType.DMA((4,)),
        ],
        compiler_params=pltpu.CompilerParams(
            collective_id=0, has_side_effects=True, vmem_limit_bytes=48 * 1024 * 1024
        ),
        cost_estimate=pl.CostEstimate(
            flops=16_000_000_000, bytes_accessed=30_000_000, transcendentals=0
        ),
    )(*(pltpu.with_memory_space_constraint(a, pltpu.HBM) for a in (coupling, spectra)), table, np.ascontiguousarray(table.T))


def solution(mesh):
    return jax.shard_map(
        on_device,
        mesh=mesh,
        in_specs=(P("row", None, "col"), P()),
        out_specs=P("row", None, "col"),
        check_vma=False,
    )
```

```python
import functools
import math

import jax
import jax.numpy as jnp
import ml_dtypes
import numpy as np
from jax import lax
from jax.experimental import pallas as pl
from jax.experimental.pallas import tpu as pltpu
from jax.sharding import PartitionSpec as P

MESH = pl.DeviceIdType.MESH
N = 3072
M = 1024
MODES = 2 * M
EARLY = 1
GROUPS = ((0, 1, 2), (3,))
NQ = 3
LINES = N // (16 * NQ)
ROWS = 16 * LINES
TILE = 256


def fourier_table():
    point = np.arange(N, dtype=np.int64)
    wave = np.arange(1, M + 1, dtype=np.int64)
    angle = (point[:, None] * wave[None, :] % N).astype(np.float64) * (2.0 * math.pi / N)
    table = np.concatenate([np.cos(angle), np.sin(angle)], 1) / math.sqrt(M)
    return table.astype(ml_dtypes.bfloat16)


def device_at(y, z, x, core):
    return (y * 2 + z % 2, z // 2 * 8 + x * 2 + core)


def round_trip(
    coupling_hbm, spectra, by_point, by_mode, out,
    coupling, spec, points, modes, sent1, got1, lines, tend, sent2, got2, total,
    load_sem, send_sem, recv_sem, last_sem,
):
    row, col = lax.axis_index("row"), lax.axis_index("col")
    y, parity = row // 2, row % 2
    z_hi, x, core = col // 8, col // 2 % 4, col % 2
    other = 1 - parity
    mine = x * 4 + z_hi * 2 + core
    z = z_hi * 2 + parity

    def x_at(i):
        return (x + (1, 3, 2, 0)[i]) % 4

    def z_at(up):
        return (z + 1 + 2 * (up % 2)) % 4 // 2

    def partner(xp, zp, cp):
        return device_at(y, zp * 2 + other, xp, cp)

    loads = [
        pltpu.make_async_copy(spectra.at[f], spec.at[:, pl.ds(f * 128, 128)], load_sem.at[f])
        for f in range(2)
    ]
    for i in range(4):
        first = pl.ds(pl.multiple_of(x_at(i) * 4 * LINES, 4 * LINES), 4 * LINES)
        loads.append(
            pltpu.make_async_copy(by_point.at[first], points.at[first], load_sem.at[2 + i])
        )
    loads += [
        pltpu.make_async_copy(
            by_point.at[pl.ds(q * ROWS, ROWS)], points.at[pl.ds(q * ROWS, ROWS)], load_sem.at[5 + q]
        )
        for q in range(1, NQ)
    ]
    loads.append(pltpu.make_async_copy(by_mode, modes, load_sem.at[5 + NQ]))
    loads.append(pltpu.make_async_copy(coupling_hbm, coupling, load_sem.at[6 + NQ]))
    for load in loads:
        load.start()

    barrier = pltpu.get_barrier_semaphore()
    for xp in range(4):
        for zp in range(2):
            for cp in range(2):
                pl.semaphore_signal(
                    barrier, inc=1, device_id=partner(xp, zp, cp), device_id_type=MESH
                )
    loads[0].wait()
    loads[1].wait()

    def whole(leg, q):
        sent, got = ((sent1, got1), (sent2, got2))[leg]
        return pltpu.make_async_remote_copy(
            sent.at[q], got.at[q], send_sem.at[leg, q], recv_sem.at[leg, q],
            device_id=partner(x, 0, core), device_id_type=MESH,
        )

    def last_part(xs):
        return pltpu.make_async_remote_copy(
            sent2.at[NQ - 1, pl.ds(0, 4)], got2.at[NQ - 1, pl.ds(xs * 4, 4)],
            send_sem.at[1, NQ - 1], last_sem.at[xs],
            device_id=partner(x, 0, core), device_id_type=MESH,
        )

    def to_rows(q, i):
        xo = x_at(i)
        start = pl.multiple_of(q * ROWS + xo * 4 * LINES, 4 * LINES)
        half = jnp.dot(
            points[pl.ds(start, 4 * LINES), :], spec[...], preferred_element_type=jnp.float32
        ).astype(jnp.bfloat16)
        sent1[q, pl.ds(xo * 4, 4)] = half.reshape(4, LINES, 256)

    def send_rows(q, i, up):
        xo, zo = x_at(i), z_at(up)
        for co in range(2):
            pltpu.make_async_remote_copy(
                sent1.at[q, xo * 4 + zo * 2 + co], got1.at[q, col],
                send_sem.at[0, q], recv_sem.at[0, q],
                device_id=partner(xo, zo, co), device_id_type=MESH,
            ).start()

    for i in range(EARLY):
        loads[2 + i].wait()
        to_rows(0, i)
    pl.semaphore_wait(barrier, 16)
    for up in range(2):
        for i in range(EARLY):
            send_rows(0, i, i + up)
    for i in range(EARLY, 4):
        loads[2 + i].wait()
        to_rows(0, i)
        send_rows(0, i, i)
        send_rows(0, i, i + 1)
    for q in range(1, NQ):
        loads[5 + q].wait()
        for i in range(4):
            to_rows(q, i)
        for up in range(2):
            for i in range(4):
                send_rows(q, i, i + up)

    loads[5 + NQ].wait()
    loads[6 + NQ].wait()
    field = (y * 2 + other) * 2
    strengths = (coupling[field], coupling[field + 1])

    for q in range(NQ):
        whole(0, q).wait_recv()
        for f in range(2):
            for s in range(16):
                lines[f * LINES : (f + 1) * LINES, s * 128 : (s + 1) * 128] = got1[
                    q, s, :, f * 128 : (f + 1) * 128
                ]

        @pl.loop(0, N // TILE, unroll=4)
        def _(n):
            cols = pl.ds(pl.multiple_of(n * TILE, TILE), TILE)
            grid = jnp.dot(lines[...], modes[:, cols], preferred_element_type=jnp.float32)
            for f in range(2):
                g = grid[f * LINES : (f + 1) * LINES]
                tend[f * LINES : (f + 1) * LINES, cols] = (g + strengths[f] * g * g).astype(
                    jnp.bfloat16
                )

        def to_modes(h, i):
            zd, xd = z_at(h + i), x_at(i)
            n = zd * 4 + xd
            cols = pl.ds(pl.multiple_of(n * TILE, TILE), TILE)
            back = jnp.dot(tend[...], points[:, cols], preferred_element_type=jnp.float32)
            back = (back * (2.0 / 3.0)).astype(jnp.bfloat16)
            for cd in range(2):
                for f in range(2):
                    sent2[q, 2 * n + cd, :, f * 128 : (f + 1) * 128] = back[
                        f * LINES : (f + 1) * LINES, cd * 128 : (cd + 1) * 128
                    ]

        def send_modes(h, i):
            zd, xd = z_at(h + i), x_at(i)
            n = zd * 4 + xd
            for cd in (1, 0):
                pltpu.make_async_remote_copy(
                    sent2.at[q, 2 * n + cd], got2.at[q, mine],
                    send_sem.at[1, q], last_sem.at[x] if q == NQ - 1 else recv_sem.at[1, q],
                    device_id=partner(xd, zd, cd), device_id_type=MESH,
                ).start()

        @pl.loop(0, 2)
        def _(h):
            for pair in (0, 2):
                for i in range(2):
                    to_modes(h, pair + i)
                for i in range(2):
                    send_modes(h, pair + i)

    kx = (col * 128 + lax.broadcasted_iota(jnp.int32, (1, 128), 1)) % M + 1

    def finish(rows, start, part):
        part = (part * (2.0 / 3.0)).astype(jnp.bfloat16)
        ky = (start + lax.broadcasted_iota(jnp.int32, (TILE, 1), 0)) % M + 1
        inside = kx * kx + ky * ky <= M * M
        for f in range(2):
            kept = jnp.where(inside, part[:, f * 128 : (f + 1) * 128], 0.0)
            out[f, rows, :] = kept.astype(jnp.bfloat16)

    for q in range(NQ - 1):
        whole(1, q).wait_recv()

        @pl.loop(0, MODES // TILE, unroll=4)
        def _(m):
            rows = pl.ds(pl.multiple_of(m * TILE, TILE), TILE)
            part = jnp.dot(
                modes[rows, q * ROWS : (q + 1) * ROWS],
                got2[q].reshape(ROWS, 256),
                preferred_element_type=jnp.float32,
            )
            if q > 0:
                part = part + total[rows, :]
            total[rows, :] = part

    for group in GROUPS:
        pieces = [(x + (3, 1, 2, 0)[j]) % 4 for j in group]
        for xs in pieces:
            last_part(xs).wait_recv()

        @pl.loop(0, MODES // TILE, unroll=8)
        def _(m):
            start = pl.multiple_of(m * TILE, TILE)
            rows = pl.ds(start, TILE)
            part = total[rows, :]
            for xs in pieces:
                first = pl.multiple_of((NQ - 1) * ROWS + xs * 4 * LINES, 4 * LINES)
                part += jnp.dot(
                    modes[rows, pl.ds(first, 4 * LINES)],
                    got2[NQ - 1, pl.ds(xs * 4, 4)].reshape(4 * LINES, 256),
                    preferred_element_type=jnp.float32,
                )
            if group != GROUPS[-1]:
                total[rows, :] = part
            else:
                finish(rows, start, part)

    for q in range(NQ):
        whole(0, q).wait_send()
        whole(1, q).wait_send()


def on_device(spectra, coupling):
    table = fourier_table()
    in_hbm = pl.BlockSpec(memory_space=pltpu.HBM)
    return pl.pallas_call(
        round_trip,
        out_shape=jax.ShapeDtypeStruct(spectra.shape, jnp.bfloat16),
        in_specs=[in_hbm] * 4,
        out_specs=pl.BlockSpec(memory_space=pltpu.VMEM),
        scratch_shapes=[
            pltpu.SMEM((16,), jnp.float32),
            pltpu.VMEM((MODES, 256), jnp.bfloat16),
            pltpu.VMEM((N, MODES), jnp.bfloat16),
            pltpu.VMEM((MODES, N), jnp.bfloat16),
            pltpu.VMEM((NQ, 16, LINES, 256), jnp.bfloat16),
            pltpu.VMEM((NQ, 16, LINES, 256), jnp.bfloat16),
            pltpu.VMEM((2 * LINES, MODES), jnp.bfloat16),
            pltpu.VMEM((2 * LINES, N), jnp.bfloat16),
            pltpu.VMEM((NQ, 16, LINES, 256), jnp.bfloat16),
            pltpu.VMEM((NQ, 16, LINES, 256), jnp.bfloat16),
            pltpu.VMEM((MODES, 256), jnp.float32),
            pltpu.SemaphoreType.DMA((7 + NQ,)),
            pltpu.SemaphoreType.DMA((2, NQ)),
            pltpu.SemaphoreType.DMA((2, NQ)),
            pltpu.SemaphoreType.DMA((4,)),
        ],
        compiler_params=pltpu.CompilerParams(
            collective_id=0, has_side_effects=True, vmem_limit_bytes=48 * 1024 * 1024
        ),
        cost_estimate=pl.CostEstimate(
            flops=16_000_000_000, bytes_accessed=30_000_000, transcendentals=0
        ),
    )(*(pltpu.with_memory_space_constraint(a, pltpu.HBM) for a in (coupling, spectra)), table, np.ascontiguousarray(table.T))


def solution(mesh):
    return jax.shard_map(
        on_device,
        mesh=mesh,
        in_specs=(P("row", None, "col"), P()),
        out_specs=P("row", None, "col"),
        check_vma=False,
    )
```
